8 devices in a mesh: part: 1 (over z), row: 2 (over y), col: 2 (over x), dep: 2 (over core).
Axes of the slice: x: 2, y: 2, z: 1, core: 2. Of those that a mesh axis runs over, the one named last changes fastest.
Arguments:
- x_in: bfloat16 [4096, 2560], P(('part', 'row', 'col'), 'dep')
- ln_scale: float32 [2560], P('dep')
- ln_shift: float32 [2560], P('dep')
- w_up: bfloat16 [2560, 10240], P(('dep', 'row'), 'col')
- b_up: bfloat16 [10240], P('col')
- w_down: bfloat16 [10240, 2560], P(('col', 'row'), 'dep')
- b_down: bfloat16 [2560], P('dep')
- y_grad: bfloat16 [4096, 2560], P(('part', 'row', 'col'), 'dep')
Outputs:
- output 1: bfloat16 [4096, 2560], P(('part', 'row', 'col'), 'dep')
- output 2: bfloat16 [4096, 2560], P(('part', 'row', 'col'), 'dep')
- output 3: bfloat16 [2560, 10240], P(('part', 'dep', 'row'), 'col')
- output 4: float32 [10240], P(('part', 'col'))
- output 5: bfloat16 [10240, 2560], P(('part', 'col', 'row'), 'dep')
- output 6: float32 [2560], P(('part', 'dep'))
- output 7: float32 [2560], P(('part', 'dep'))
- output 8: float32 [2560], P(('part', 'dep'))
All inputs are finite; a program needn't handle non-finite values.
Results may differ from the reference program's by a relative error of at most 0.00149.
Values are sent between devices in bfloat16 or wider.
A program may use at most 1 GiB of HBM per device.

```python
import jax
import jax.numpy as jnp
from jax import lax

TOKENS = 4096
D_MODEL = 2560
D_FF = 10240

BLOCK_ROWS = min(TOKENS, 512)
N_BLOCKS = TOKENS // BLOCK_ROWS
LN_EPS = 1e-5
GELU_K = 0.7978845608028654
GELU_C = 0.044715
TWO_PI = 6.283185307179586


def setup_inputs(seed: int = 0, part: int = 0) -> dict:
    shared_root, part_root = jax.random.split(jax.random.key(seed))
    part_keys = jax.random.split(jax.random.fold_in(part_root, part), 4)
    shared_keys = jax.random.split(shared_root, 6)
    col_pos = jnp.arange(D_MODEL, dtype=jnp.float32) / D_MODEL
    col_phase = jax.random.uniform(part_keys[0], (), jnp.float32, 0.0, TWO_PI)
    col_mean = 1.5 * jnp.sin(TWO_PI * col_pos + col_phase) + 0.5 * jax.random.normal(part_keys[1], (D_MODEL,), jnp.float32)
    x_vals = jax.random.normal(part_keys[2], (TOKENS, D_MODEL), jnp.float32) + col_mean
    g_vals = jax.random.normal(part_keys[3], (TOKENS, D_MODEL), jnp.float32)
    return {
        "x_in": x_vals.astype(jnp.bfloat16),
        "ln_scale": 1.0 + 0.3 * jax.random.normal(shared_keys[0], (D_MODEL,), jnp.float32),
        "ln_shift": 0.5 * jax.random.normal(shared_keys[1], (D_MODEL,), jnp.float32),
        "w_up": (jax.random.normal(shared_keys[2], (D_MODEL, D_FF), jnp.float32) * D_MODEL ** -0.5).astype(jnp.bfloat16),
        "b_up": (0.5 * jax.random.normal(shared_keys[3], (D_FF,), jnp.float32)).astype(jnp.bfloat16),
        "w_down": (jax.random.normal(shared_keys[4], (D_FF, D_MODEL), jnp.float32) * D_FF ** -0.5).astype(jnp.bfloat16),
        "b_down": (0.5 * jax.random.normal(shared_keys[5], (D_MODEL,), jnp.float32)).astype(jnp.bfloat16),
        "y_grad": g_vals.astype(jnp.bfloat16),
    }


def gelu_tanh(pre_act):
    inner_arg = GELU_K * (pre_act + GELU_C * pre_act * (pre_act * pre_act))
    return 0.5 * pre_act * (1.0 + jnp.tanh(inner_arg))


def gelu_slope(pre_act):
    squared = pre_act * pre_act
    tanh_val = jnp.tanh(GELU_K * (pre_act + GELU_C * pre_act * squared))
    return 0.5 * (1.0 + tanh_val) + 0.5 * pre_act * (1.0 - tanh_val * tanh_val) * GELU_K * (1.0 + 3.0 * GELU_C * squared)


def block_pass(x_blk, g_blk, ln_scale, ln_shift, w_up, b_up, w_down, b_down):
    x_float = x_blk.astype(jnp.float32)
    mean_row = jnp.sum(x_float, axis=1, keepdims=True) / D_MODEL
    var_row = jnp.sum(x_float * x_float, axis=1, keepdims=True) / D_MODEL - mean_row * mean_row
    inv_std = lax.rsqrt(var_row + LN_EPS)
    x_hat = (x_float - mean_row) * inv_std
    normed = (x_hat * ln_scale + ln_shift).astype(jnp.bfloat16)
    pre_act = jnp.dot(normed, w_up, preferred_element_type=jnp.float32) + b_up.astype(jnp.float32)
    hidden = gelu_tanh(pre_act).astype(jnp.bfloat16)
    out_sum = jnp.dot(hidden, w_down, preferred_element_type=jnp.float32)
    y_blk = (x_float + out_sum + b_down.astype(jnp.float32)).astype(jnp.bfloat16)
    g_float = g_blk.astype(jnp.float32)
    w_down_part = jnp.dot(hidden.T, g_blk, preferred_element_type=jnp.float32)
    hid_grad = jnp.dot(g_blk, w_down.T, preferred_element_type=jnp.float32)
    pre_grad = hid_grad * gelu_slope(pre_act)
    pre_lowp = pre_grad.astype(jnp.bfloat16)
    w_up_part = jnp.dot(normed.T, pre_lowp, preferred_element_type=jnp.float32)
    norm_grad = jnp.dot(pre_lowp, w_up.T, preferred_element_type=jnp.float32)
    xhat_grad = norm_grad * ln_scale
    mean_one = jnp.sum(xhat_grad, axis=1, keepdims=True) / D_MODEL
    mean_two = jnp.sum(xhat_grad * x_hat, axis=1, keepdims=True) / D_MODEL
    dx_blk = (g_float + inv_std * (xhat_grad - mean_one - x_hat * mean_two)).astype(jnp.bfloat16)
    part_sums = (w_up_part, jnp.sum(pre_grad, axis=0), w_down_part, jnp.sum(g_float, axis=0), jnp.sum(norm_grad * x_hat, axis=0), jnp.sum(norm_grad, axis=0))
    return y_blk, dx_blk, part_sums


def reference(x_in, ln_scale, ln_shift, w_up, b_up, w_down, b_down, y_grad):
    x_blocks = x_in.reshape(N_BLOCKS, BLOCK_ROWS, D_MODEL)
    g_blocks = y_grad.reshape(N_BLOCKS, BLOCK_ROWS, D_MODEL)

    def scan_step(acc_sums, blk_pair):
        y_blk, dx_blk, part_sums = block_pass(blk_pair[0], blk_pair[1], ln_scale, ln_shift, w_up, b_up, w_down, b_down)
        new_sums = tuple(acc_val + add_val for acc_val, add_val in zip(acc_sums, part_sums))
        return new_sums, (y_blk, dx_blk)

    zero_sums = (jnp.zeros((D_MODEL, D_FF), jnp.float32), jnp.zeros((D_FF,), jnp.float32), jnp.zeros((D_FF, D_MODEL), jnp.float32), jnp.zeros((D_MODEL,), jnp.float32), jnp.zeros((D_MODEL,), jnp.float32), jnp.zeros((D_MODEL,), jnp.float32))
    total_sums, out_blocks = lax.scan(scan_step, zero_sums, (x_blocks, g_blocks))
    return (out_blocks[0].reshape(TOKENS, D_MODEL), out_blocks[1].reshape(TOKENS, D_MODEL), total_sums[0].astype(jnp.bfloat16), total_sums[1], total_sums[2].astype(jnp.bfloat16), total_sums[3], total_sums[4], total_sums[5])
```

```python
import functools
import jax
import jax.numpy as jnp
from jax import lax
from jax.experimental import pallas as pl
from jax.experimental.pallas import tpu as pltpu
from jax.sharding import PartitionSpec as P

LN_EPS = 1e-5
GELU_K = 0.7978845608028654
GELU_C = 0.044715
SWAP = [(0, 1), (1, 0)]
CROSS = [(0, 3), (1, 2), (2, 1), (3, 0)]
f32 = jnp.float32
bf16 = jnp.bfloat16
VMEM_LIMIT = 60 * 1024 * 1024
CH_ACT = 256
CH_OUT = 1280
CH_GRAD = 256


def gelu_both(c):
    sq = c * c
    t = jnp.tanh(c * (GELU_K + (GELU_K * GELU_C) * sq))
    half = 0.5 * c
    h = half + half * t
    s = (0.5 + 0.5 * t) + half * (1.0 - t * t) * (GELU_K + (3.0 * GELU_K * GELU_C) * sq)
    return h, s


def mm(a, b):
    return lax.dot_general(a, b, (((1,), (0,)), ((), ())), preferred_element_type=f32)


def mmt(a, b):
    return lax.dot_general(a, b, (((1,), (1,)), ((), ())), preferred_element_type=f32)


def side(u, v):
    return jnp.concatenate([u[...], v[...]], axis=1)


def run_copies(copies, sems):
    descs = [pltpu.make_async_copy(s, d, sems.at[i]) for i, (s, d) in enumerate(copies)]
    for c in descs:
        c.start()
    for c in descs:
        c.wait()


def tile_map(b, nb, i, *_):
    return (jnp.clip(i - b * nb, 0, nb - 1), 0)


HBM = pl.BlockSpec(memory_space=pl.ANY)


def tiled_call(body, idx, blocks_in, weights, consts, blocks_out, sums_out, scratch, bm, flops):
    nblk = len(blocks_in)
    n = blocks_in[0][0].shape[0]
    nb = n // bm
    ins, in_specs, outs, out_specs = [], [], [], []
    for b, arrs in enumerate(blocks_in):
        for a in arrs:
            ins.append(a)
            in_specs.append(pl.BlockSpec((bm, a.shape[1]), functools.partial(tile_map, b, nb)))
    for w in weights:
        ins.append(w)
        in_specs.append(HBM)
    for c in consts:
        ins.append(c)
        in_specs.append(pl.BlockSpec(c.shape, lambda i, *_: (0, 0)))
    for b in range(nblk):
        for shp in blocks_out:
            outs.append(jax.ShapeDtypeStruct((n, shp[0]), shp[1]))
            out_specs.append(pl.BlockSpec((bm, shp[0]), functools.partial(tile_map, b, nb)))
    for shp in sums_out:
        outs.append(jax.ShapeDtypeStruct(shp, f32))
        out_specs.append(pl.BlockSpec(shp, lambda i, *_: (0, 0)))
    na, no = len(blocks_in[0]), len(blocks_out)

    def kernel(idx_ref, *refs):
        i = pl.program_id(0)
        at = 0
        tin = [refs[b * na:(b + 1) * na] for b in range(nblk)]
        at = na * nblk
        wr = refs[at:at + len(weights)]
        at += len(weights)
        cr = refs[at:at + len(consts)]
        at += len(consts)
        tout = [refs[at + b * no:at + (b + 1) * no] for b in range(nblk)]
        at += no * nblk
        sr = refs[at:at + len(sums_out)]
        at += len(sums_out)
        scr, sems = refs[at:-1], refs[-1]
        load, step = body

        @pl.when(i == 0)
        def _():
            run_copies(load(idx_ref[0], idx_ref[1], wr, scr), sems)
            for s in sr:
                s[...] = jnp.zeros_like(s)

        for b in range(nblk):
            @pl.when(i // nb == b)
            def _(b=b):
                step(tin[b], cr, tout[b], sr, scr)

    call = pl.pallas_call(
        kernel,
        out_shape=outs,
        grid_spec=pltpu.PrefetchScalarGridSpec(
            num_scalar_prefetch=1, grid=(nblk * nb,), in_specs=in_specs, out_specs=out_specs,
            scratch_shapes=list(scratch) + [pltpu.SemaphoreType.DMA((32,))]),
        compiler_params=pltpu.CompilerParams(dimension_semantics=("arbitrary",), vmem_limit_bytes=VMEM_LIMIT),
        cost_estimate=pl.CostEstimate(flops=flops, bytes_accessed=1 << 24, transcendentals=0),
    )
    return call(idx, *ins)


def col_at(ref, start, size):
    return ref.at[:, pl.ds(pl.multiple_of(start, 128), size)]


def row_at(ref, start, size):
    return ref.at[pl.ds(pl.multiple_of(start, 8), size), :]


def act_call(mode, idx, blocks, groups, w_up, w_down, biases, bm, with_sums):
    fe = w_up.shape[1] // 4
    q = w_up.shape[0]
    dm = 4 * q
    ng = len(groups)
    has_c, has_d = "c" in mode, "d" in mode
    weights = [w_up, w_down]
    for _, p1, p2 in groups:
        weights += (list(p1) if has_c else []) + (list(p2) if has_d else [])

    def load(r, k, wr, scr):
        up, down = wr[0], wr[1]
        rest = list(wr[2:])
        bufs = list(scr)
        copies = []
        for own, p1, p2 in groups:
            if has_c:
                buf = bufs.pop(0)
                rr = r if own else 1 - r
                dep, row, cross = rest.pop(0), rest.pop(0), rest.pop(0)
                copies += [(col_at(up, (rr * 2 + k) * fe, fe), row_at(buf, r * q, q)),
                           (row, row_at(buf, (1 - r) * q, q)),
                           (dep, row_at(buf, 2 * q + r * q, q)),
                           (cross, row_at(buf, 2 * q + (1 - r) * q, q))]
            if has_d:
                buf = bufs.pop(0)
                if own:
                    dep = rest.pop(0)
                    copies += [(row_at(down, k * fe, fe), buf.at[:, 0:2 * q]), (dep, buf.at[:, 2 * q:4 * q])]
                else:
                    for j in range(4):
                        copies.append((rest.pop(0), buf.at[:, j * q:(j + 1) * q]))
        return copies

    def step(tin, cr, tout, sr, scr):
        tin, bufs = list(tin), list(scr)
        u, v = (tin.pop(0), tin.pop(0)) if has_c else (None, None)
        gu, gv = (tin.pop(0), tin.pop(0)) if has_d else (None, None)
        tout = list(tout)
        for g in range(ng):
            w1 = bufs.pop(0) if has_c else None
            w2 = bufs.pop(0) if has_d else None
            s_in = tin.pop(0) if not has_c else None
            h_out = tout.pop(0) if has_c else None
            x_out = tout.pop(0)
            for n0 in range(0, fe, CH_ACT):
                sl = slice(n0, n0 + CH_ACT)
                if has_c:
                    c = mm(side(u, v), w1[:, sl]) + cr[g][:, sl]
                    h, s = gelu_both(c)
                    h_out[:, sl] = h.astype(bf16)
                else:
                    s = s_in[:, sl]
                if has_d:
                    p = mmt(side(gu, gv), w2[sl, :]) * s
                    x_out[:, sl] = p.astype(bf16)
                    if with_sums:
                        sr[g][:, sl] += jnp.sum(p, axis=0, keepdims=True)
                else:
                    x_out[:, sl] = s

    scratch = []
    for _ in range(ng):
        scratch += [pltpu.VMEM((dm, fe), bf16)] if has_c else []
        scratch += [pltpu.VMEM((fe, dm), bf16)] if has_d else []
    outs = []
    for _ in range(ng):
        outs += [(fe, bf16)] if has_c else []
        outs += [(fe, bf16)] if has_d else [(fe, f32)]
    n = blocks[0][0].shape[0]
    flops = 2 * n * len(blocks) * dm * fe * ng * (int(has_c) + int(has_d))
    res = tiled_call((load, step), idx, blocks, weights, [b.reshape(1, fe) for b in biases] if has_c else [],
                     outs, [(1, fe)] * ng if with_sums else [], scratch, bm, flops)
    no = len(outs)
    per = [res[b * no:(b + 1) * no] for b in range(len(blocks))]
    return per, res[no * len(blocks):]


def out_call(idx, blocks, weights, load_fn, transposed, q, fe, bm):
    shape = (2 * q, 2 * fe) if transposed else (2 * fe, 2 * q)

    def load(r, k, wr, scr):
        return load_fn(r, k, wr, scr[0])

    def step(tin, cr, tout, sr, scr):
        o, n = tin
        w = scr[0]
        for n0 in range(0, 2 * q, CH_OUT):
            n1 = n0 + CH_OUT
            y = mmt(side(o, n), w[n0:n1, :]) if transposed else mm(side(o, n), w[:, n0:n1])
            if n0 < q:
                tout[0][:, n0:min(n1, q)] = y[:, :min(n1, q) - n0]
            if n1 > q:
                m = max(q - n0, 0)
                tout[1][:, n0 + m - q:n1 - q] = y[:, m:]

    flops = 2 * blocks[0][0].shape[0] * len(blocks) * 2 * q * 2 * fe
    res = tiled_call((load, step), idx, blocks, weights, [], [(q, f32), (q, f32)], [], [pltpu.VMEM(shape, bf16)], bm, flops)
    return [res[2 * b:2 * b + 2] for b in range(len(blocks))]


def grad_call(idx, lhs, rhs, acc, out_dtype, halves):
    nblk = len(rhs)
    n = rhs[0][0].shape[0]
    fe = rhs[0][0].shape[1]
    m = fe
    ng = len(rhs[0])
    nt = fe // CH_GRAD
    ins, in_specs = [], []
    for parts in lhs:
        for p in parts:
            ins.append(p)
            if halves:
                in_specs.append(pl.BlockSpec((n, m // 2), lambda j, s: (0, s[0]), pipeline_mode=pl.Buffered(1)))
            else:
                in_specs.append(pl.BlockSpec((n, m), lambda j, s: (0, 0), pipeline_mode=pl.Buffered(1)))
    for parts in rhs:
        for p in parts:
            ins.append(p)
            in_specs.append(pl.BlockSpec((n, CH_GRAD), lambda j, s: (0, j)))
    for p in acc:
        ins.append(p)
        in_specs.append(pl.BlockSpec((m, CH_GRAD), lambda j, s: (0, j)))
    nl = len(lhs[0])

    def kernel(idx_ref, *refs):
        lr = refs[:nl * nblk]
        rr = refs[nl * nblk:nl * nblk + ng * nblk]
        ar = refs[nl * nblk + ng * nblk:nl * nblk + ng * nblk + len(acc)]
        outs, scr = refs[-1 - ng:-1], refs[-1]

        @pl.when(pl.program_id(0) == 0)
        def _():
            for b in range(nblk):
                for p in range(nl):
                    w = m // nl
                    scr[p * w:(p + 1) * w, b * n:(b + 1) * n] = lr[b * nl + p][...].T

        for g in range(ng):
            y = mm(scr[...], jnp.concatenate([rr[b * ng + g][...] for b in range(nblk)], axis=0))
            if acc:
                y = y + ar[g][...]
            outs[g][...] = y.astype(out_dtype)

    res = pl.pallas_call(
        kernel,
        out_shape=[jax.ShapeDtypeStruct((m, fe), out_dtype)] * ng,
        grid_spec=pltpu.PrefetchScalarGridSpec(
            num_scalar_prefetch=1, grid=(nt,), in_specs=in_specs,
            out_specs=[pl.BlockSpec((m, CH_GRAD), lambda j, s: (0, j))] * ng,
            scratch_shapes=[pltpu.VMEM((m, nblk * n), bf16)]),
        compiler_params=pltpu.CompilerParams(dimension_semantics=("arbitrary",), vmem_limit_bytes=VMEM_LIMIT),
        cost_estimate=pl.CostEstimate(flops=2 * n * nblk * m * fe * ng, bytes_accessed=1 << 24, transcendentals=0),
    )(idx, *ins)
    return res


def solution(mesh):
    dep_size = mesh.shape["dep"]
    tok_spec = P(("part", "row", "col"), "dep")
    vec_dep = P("dep")
    part_dep = P(("part", "dep"))
    in_specs = (tok_spec, vec_dep, vec_dep, P(("dep", "row"), "col"), P("col"), P(("col", "row"), "dep"), vec_dep, tok_spec)
    out_specs = (tok_spec, tok_spec, P(("part", "dep", "row"), "col"), P(("part", "col")), P(("part", "col", "row"), "dep"), part_dep, part_dep, part_dep)

    def px(v):
        return lax.ppermute(v, "col", SWAP)

    def py(v):
        return lax.ppermute(v, "row", SWAP)

    def pd(v):
        return lax.ppermute(v, "dep", SWAP)

    def pyd(v):
        return lax.ppermute(v, ("row", "dep"), CROSS)

    def local_step(x_in, ln_scale, ln_shift, w_up, b_up, w_down, b_down, y_grad):
        r = lax.axis_index("row")
        k = lax.axis_index("dep")
        idx = jnp.stack([r, k]).astype(jnp.int32)
        _, dh_ = x_in.shape
        q = dh_ // 2
        fe = w_up.shape[1] // 4
        row_width = dh_ * dep_size

        def cols(rr, kk):
            return lax.dynamic_slice_in_dim(w_up, (rr * 2 + kk) * fe, fe, axis=1)

        def rows(kk):
            return lax.dynamic_slice_in_dim(w_down, kk * fe, fe, axis=0)

        def bias(rr):
            return lax.dynamic_slice_in_dim(b_up, (rr * 2 + k) * fe, fe, axis=0).astype(f32)

        gx = px(y_grad)
        own_o, own_n, snd_o, snd_n = cols(r, k), cols(1 - r, k), cols(r, 1 - k), cols(1 - r, 1 - k)
        w1o = (pd(snd_o), py(own_n), pyd(snd_n))
        w1n = (pd(snd_n), py(own_o), pyd(snd_o))
        rk, rk2 = rows(k), rows(1 - k)
        w2o = (pd(rk2),)
        own0, oth0 = py(rk[:, :q]), pyd(rk2[:, :q])
        own1, oth1 = py(rk[:, q:]), pyd(rk2[:, q:])
        w2n = (own0, own1, oth0, oth1)
        bo, bn = bias(r), bias(1 - r)

        x_float = x_in.astype(f32)
        row_stats = jnp.stack([jnp.sum(x_float, axis=1), jnp.sum(x_float * x_float, axis=1)], axis=1)
        row_stats = lax.psum(row_stats, "dep")
        mean_row = row_stats[:, 0:1] / row_width
        var_row = row_stats[:, 1:2] / row_width - mean_row * mean_row
        inv_std = lax.rsqrt(var_row + LN_EPS)
        x_hat = (x_float - mean_row) * inv_std
        a0 = (x_hat * ln_scale + ln_shift).astype(bf16)
        ax, ay = px(a0), py(a0)
        gy = py(y_grad)
        ad, gd = py(ax), px(gy)

        def half(u):
            return (u, pd(u))

        A = [half(a0), half(ax), half(ay), half(ad)]
        G = [half(y_grad), half(gx), half(gy), half(gd)]
        go, gn = (True, w1o, w2o), (False, w1n, w2n)

        def act(mode, blocks, groups, biases, bm, sums):
            return act_call(mode, idx, blocks, groups, w_up, w_down, biases, bm, sums)

        (o0, ox), (sum_o,) = act("cd", [A[0] + G[0], A[1] + G[1]], [go], [bo], 512, True)
        (n0, nx), _ = act("c", [A[0], A[1]], [gn], [bn], 512, False)
        dw2 = grad_call(idx, [[o0[0]], [ox[0]]], [G[0], G[1]], [], f32, False)
        dw1o = grad_call(idx, [A[0], A[1]], [[o0[1]], [ox[1]]], [], f32, True)

        def reduce_out(parts):
            (own_a, oth_a), (own_x, oth_x) = parts
            send = own_x + pd(oth_x)
            return own_a + pd(oth_a) + px(send)

        def y_load(j):
            def load(rr, kk, wr, buf):
                down, dep, a, b = wr
                return [(down.at[pl.ds(pl.multiple_of(kk * fe, 8), fe), j * q:(j + 1) * q], buf.at[0:fe, 0:q]),
                        (dep.at[:, j * q:(j + 1) * q], buf.at[0:fe, q:2 * q]),
                        (a, buf.at[fe:2 * fe, 0:q]), (b, buf.at[fe:2 * fe, q:2 * q])]

            return load

        hs = [(o0[0], n0[0]), (ox[0], nx[0])]
        y_parts = []
        for j, (own, oth) in enumerate(((own0, oth0), (own1, oth1))):
            res = out_call(idx, hs, [w_down, w2o[0], own, oth], y_load(j), False, q, fe, 512)
            y_parts.append(reduce_out(res))
        y_out = (x_float + jnp.concatenate(y_parts, axis=1) + b_down.astype(f32)).astype(bf16)

        (m0, mx), (sum_n,) = act("d", [tuple(G[0]) + (n0[1],), tuple(G[1]) + (nx[1],)], [gn], [], 512, True)

        def da_load_own(rr, kk, wr, buf):
            up, do, dn = wr
            return [(col_at(up, (rr * 2 + kk) * fe, fe), buf.at[0:q, 0:fe]), (col_at(up, ((1 - rr) * 2 + kk) * fe, fe), buf.at[0:q, fe:2 * fe]),
                    (do, buf.at[q:2 * q, 0:fe]), (dn, buf.at[q:2 * q, fe:2 * fe])]

        def da_load_oth(rr, kk, wr, buf):
            a, b, do, dn = wr
            return [(a, buf.at[0:q, 0:fe]), (b, buf.at[0:q, fe:2 * fe]), (do, buf.at[q:2 * q, 0:fe]), (dn, buf.at[q:2 * q, fe:2 * fe])]

        ds = [(o0[1], m0[0]), (ox[1], mx[0])]
        res = out_call(idx, ds, [w_up, w1o[0], w1n[0]], da_load_own, True, q, fe, 512)
        na = reduce_out(res)
        res = out_call(idx, ds, [w1o[1], w1n[1], w1o[2], w1n[2]], da_load_oth, True, q, fe, 512)
        nb = reduce_out(res)
        norm_grad = jnp.where(r == 0, jnp.concatenate([na, nb], axis=1), jnp.concatenate([nb, na], axis=1))
        value = norm_grad * ln_scale
        grad_stats = jnp.stack([jnp.sum(value, axis=1), jnp.sum(value * x_hat, axis=1)], axis=1)
        grad_stats = lax.psum(grad_stats, "dep")
        dx = inv_std * (value - grad_stats[:, 0:1] / row_width - x_hat * (grad_stats[:, 1:2] / row_width))
        x_grad = (y_grad.astype(f32) + dx).astype(bf16)
        gains = jnp.stack([jnp.sum(norm_grad * x_hat, axis=0), jnp.sum(norm_grad, axis=0)])

        dw1n = grad_call(idx, [A[0], A[1]], [[m0[0]], [mx[0]]], [], f32, True)
        (py_,), _ = act("cd", [A[2] + G[2]], [go, gn], [bo, bn], 256, False)
        (pz,), _ = act("cd", [A[3] + G[3]], [go, gn], [bo, bn], 256, False)
        dw2 = grad_call(idx, [[py_[0]], [pz[0]]], [G[2], G[3]], dw2, bf16, False)
        dw1o, dw1n = grad_call(idx, [A[2], A[3]], [[py_[1], py_[3]], [pz[1], pz[3]]], [dw1o[0], dw1n[0]], bf16, True)

        ro, rn = pd(dw1o[q:]), pd(dw1n[q:])
        w_up_grad = jnp.zeros(w_up.shape, bf16)
        for v, rr, kk in ((dw1o[:q], r, k), (dw1n[:q], 1 - r, k), (ro, r, 1 - k), (rn, 1 - r, 1 - k)):
            w_up_grad = lax.dynamic_update_slice_in_dim(w_up_grad, v, (rr * 2 + kk) * fe, axis=1)
        mine, other = dw2[0], pd(dw2[1])
        w_down_grad = jnp.zeros(w_down.shape, bf16)
        w_down_grad = lax.dynamic_update_slice_in_dim(w_down_grad, mine, k * fe, axis=0)
        w_down_grad = lax.dynamic_update_slice_in_dim(w_down_grad, other, (1 - k) * fe, axis=0)

        def both(v):
            v = v + px(v)
            return v + py(v)

        b_down_grad = both(jnp.sum(y_grad.astype(f32), axis=0))
        gain_sums = both(gains)
        full = jnp.concatenate([sum_o, sum_n]) + py(jnp.concatenate([sum_n, sum_o]))
        oth = pd(full)
        b_up_grad = jnp.zeros(b_up.shape, f32)
        for v, rr, kk in ((full[0], r, k), (full[1], 1 - r, k), (oth[0], r, 1 - k), (oth[1], 1 - r, 1 - k)):
            b_up_grad = lax.dynamic_update_slice_in_dim(b_up_grad, v, (rr * 2 + kk) * fe, axis=0)
        return (y_out, x_grad, w_up_grad, b_up_grad, w_down_grad, b_down_grad, gain_sums[0], gain_sums[1])

    return jax.shard_map(local_step, mesh=mesh, in_specs=in_specs, out_specs=out_specs, check_vma=False)
```

```python
import functools
import jax
import jax.numpy as jnp
from jax import lax
from jax.experimental import pallas as pl
from jax.experimental.pallas import tpu as pltpu
from jax.sharding import PartitionSpec as P

LN_EPS = 1e-5
GELU_K = 0.7978845608028654
GELU_C = 0.044715
SWAP = [(0, 1), (1, 0)]
CROSS = [(0, 3), (1, 2), (2, 1), (3, 0)]
f32 = jnp.float32
bf16 = jnp.bfloat16
VMEM_LIMIT = 60 * 1024 * 1024
CH_ACT = 256
CH_BACK = 640
CH_GRAD = 256


def gelu_both(c):
    sq = c * c
    t = jnp.tanh(c * (GELU_K + (GELU_K * GELU_C) * sq))
    half = 0.5 * c
    h = half + half * t
    s = (0.5 + 0.5 * t) + half * (1.0 - t * t) * (GELU_K + (3.0 * GELU_K * GELU_C) * sq)
    return h, s


def mm(a, b):
    return lax.dot_general(a, b, (((1,), (0,)), ((), ())), preferred_element_type=f32)


def mmt(a, b):
    return lax.dot_general(a, b, (((1,), (1,)), ((), ())), preferred_element_type=f32)


def side(u, v):
    return jnp.concatenate([u[...], v[...]], axis=1)


def copies_of(stages, sems):
    at, out = 0, []
    for stage in stages:
        out.append([pltpu.make_async_copy(s, d, sems.at[at + i]) for i, (s, d) in enumerate(stage)])
        at += len(stage)
    return out


def tile_map(b, nb, i, *_):
    return (jnp.clip(i - b * nb, 0, nb - 1), 0)


HBM = pl.BlockSpec(memory_space=pl.ANY)


def tiled_call(body, idx, pieces, flat, weights, consts, flat_out, part_out, sums_out, scratch, bm, flops):
    nblk = len(pieces)
    n = (flat[0] if flat else pieces[0][0]).shape[0] // (nblk if flat else 1)
    nb = n // bm
    ins, in_specs, outs, out_specs = [], [], [], []
    for b, arrs in enumerate(pieces):
        for a in arrs:
            ins.append(a)
            in_specs.append(pl.BlockSpec((bm, a.shape[1]), functools.partial(tile_map, b, nb)))
    for a in flat:
        ins.append(a)
        in_specs.append(pl.BlockSpec((bm, a.shape[1]), lambda i, *_: (i, 0)))
    for w in weights:
        ins.append(w)
        in_specs.append(HBM)
    for c in consts:
        ins.append(c)
        in_specs.append(pl.BlockSpec(c.shape, lambda i, *_: (0, 0)))
    for shp in flat_out:
        outs.append(jax.ShapeDtypeStruct((n * nblk, shp[0]), shp[1]))
        out_specs.append(pl.BlockSpec((bm, shp[0]), lambda i, *_: (i, 0)))
    for width in part_out:
        for b in range(nblk):
            outs.append(jax.ShapeDtypeStruct((n, width), f32))
            out_specs.append(pl.BlockSpec((bm, width), functools.partial(tile_map, b, nb)))
    for shp in sums_out:
        outs.append(jax.ShapeDtypeStruct(shp, f32))
        out_specs.append(pl.BlockSpec(shp, lambda i, *_: (0, 0)))
    na = len(pieces[0])

    def kernel(idx_ref, *refs):
        i = pl.program_id(0)
        at = na * nblk
        fl = refs[at:at + len(flat)]
        tin = [refs[b * na:(b + 1) * na] + fl for b in range(nblk)]
        at += len(flat)
        wr = refs[at:at + len(weights)]
        at += len(weights)
        cr = refs[at:at + len(consts)]
        at += len(consts)
        tout = refs[at:at + len(flat_out)]
        at += len(flat_out)
        pout = refs[at:at + len(part_out) * nblk]
        at += len(part_out) * nblk
        sr = refs[at:at + len(sums_out)]
        at += len(sums_out)
        scr, sems = refs[at:-1], refs[-1]
        load, step = body

        @pl.when(i == 0)
        def _():
            for stage in copies_of(load(idx_ref[0], idx_ref[1], wr, scr), sems):
                for c in stage:
                    c.start()
            for s in sr:
                s[...] = jnp.zeros_like(s)

        def arrive(j):
            @pl.when(i == 0)
            def _():
                for c in copies_of(load(idx_ref[0], idx_ref[1], wr, scr), sems)[j]:
                    c.wait()

        for b in range(nblk):
            @pl.when(i // nb == b)
            def _(b=b):
                step(arrive if b == 0 else lambda j: None, tin[b], cr, tout + pout[b::nblk], sr, scr)

    call = pl.pallas_call(
        kernel,
        out_shape=outs,
        grid_spec=pltpu.PrefetchScalarGridSpec(
            num_scalar_prefetch=1, grid=(nblk * nb,), in_specs=in_specs, out_specs=out_specs,
            scratch_shapes=list(scratch) + [pltpu.SemaphoreType.DMA((32,))]),
        compiler_params=pltpu.CompilerParams(dimension_semantics=("arbitrary",), vmem_limit_bytes=VMEM_LIMIT),
        cost_estimate=pl.CostEstimate(flops=flops, bytes_accessed=1 << 24, transcendentals=0),
    )
    return call(idx, *ins)


def col_at(ref, start, size):
    return ref.at[:, pl.ds(pl.multiple_of(start, 128), size)]


def row_at(ref, start, size):
    return ref.at[pl.ds(pl.multiple_of(start, 8), size), :]


def act_call(mode, idx, blocks, slopes, groups, w_up, w_down, biases, bm, with_sums):
    fe = w_up.shape[1] // 4
    q = w_up.shape[0]
    dm = 4 * q
    ng = len(groups)
    has_c, has_d = "c" in mode, "d" in mode
    weights = [w_up, w_down]
    for _, p1, p2, _ in groups:
        weights += (list(p1) if has_c else []) + (list(p2) if has_d else [])

    def load(r, k, wr, scr):
        up, down = wr[0], wr[1]
        rest = list(wr[2:])
        bufs = list(scr)
        stages = []
        for own, p1, p2, _ in groups:
            copies = []
            if has_c:
                buf = bufs.pop(0)
                rr = r if own else 1 - r
                dep, row, cross = rest.pop(0), rest.pop(0), rest.pop(0)
                copies += [(col_at(up, (rr * 2 + k) * fe, fe), row_at(buf, r * q, q)),
                           (row, row_at(buf, (1 - r) * q, q)),
                           (dep, row_at(buf, 2 * q + r * q, q)),
                           (cross, row_at(buf, 2 * q + (1 - r) * q, q))]
            if has_d:
                buf = bufs.pop(0)
                if own:
                    dep = rest.pop(0)
                    copies += [(row_at(down, k * fe, fe), buf.at[:, 0:2 * q]), (dep, buf.at[:, 2 * q:4 * q])]
                else:
                    for j in range(4):
                        copies.append((rest.pop(0), buf.at[:, j * q:(j + 1) * q]))
            stages.append(copies)
        return stages

    def step(arrive, tin, cr, tout, sr, scr):
        tin, bufs = list(tin), list(scr)
        u, v = (tin.pop(0), tin.pop(0)) if has_c else (None, None)
        gu, gv = (tin.pop(0), tin.pop(0)) if has_d else (None, None)
        tout = list(tout)
        for g in range(ng):
            arrive(g)
            w1 = bufs.pop(0) if has_c else None
            w2 = bufs.pop(0) if has_d else None
            s_in = tin.pop(0) if not has_c else None
            h_out = tout.pop(0) if has_c and groups[g][3] else None
            x_out = tout.pop(0)
            for n0 in range(0, fe, CH_ACT):
                sl = slice(n0, n0 + CH_ACT)
                if has_c:
                    c = mm(side(u, v), w1[:, sl]) + cr[g][:, sl]
                    h, s = gelu_both(c)
                    if h_out is not None:
                        h_out[:, sl] = h.astype(bf16)
                else:
                    s = s_in[:, sl]
                if has_d:
                    p = mmt(side(gu, gv), w2[sl, :]) * s
                    x_out[:, sl] = p.astype(bf16)
                    if with_sums:
                        sr[g][:, sl] += jnp.sum(p, axis=0, keepdims=True)
                else:
                    x_out[:, sl] = s

    scratch = []
    for _ in range(ng):
        scratch += [pltpu.VMEM((dm, fe), bf16)] if has_c else []
        scratch += [pltpu.VMEM((fe, dm), bf16)] if has_d else []
    outs = []
    for g in range(ng):
        outs += [(fe, bf16)] if has_c and groups[g][3] else []
        outs += [(fe, bf16)] if has_d else [(fe, f32)]
    n = blocks[0][0].shape[0]
    flops = 2 * n * len(blocks) * dm * fe * ng * (int(has_c) + int(has_d))
    res = tiled_call((load, step), idx, blocks, slopes, weights, [b.reshape(1, fe) for b in biases] if has_c else [],
                     outs, [], [(1, fe)] * ng if with_sums else [], scratch, bm, flops)
    return res


def out_call(idx, lhs, acc, weights, load_fn, q, last, bm):
    depth = sum(a.shape[1] for a in lhs)

    def load(r, k, wr, scr):
        return [load_fn(r, k, wr, scr[0])]

    def step(arrive, tin, cr, tout, sr, scr):
        arrive(0)
        y = mm(jnp.concatenate([a[...] for a in tin[:len(lhs)]], axis=1), scr[0][...])
        for p in range(2):
            v = y[:, p * q:(p + 1) * q]
            tout[p][...] = v + tin[len(lhs) + p][...] if acc else v

    flops = 2 * lhs[0].shape[0] * 2 * q * depth
    return tiled_call((load, step), idx, [(), ()], list(lhs) + list(acc), weights, [], [(q, f32)] * (1 if last else 2), [q] if last else [], [],
                      [pltpu.VMEM((depth, 2 * q), bf16)], bm, flops)


def place_rows(r, q, buf):
    mine, theirs = r * 2 * q, (1 - r) * 2 * q
    return [buf.at[pl.ds(pl.multiple_of(start, 8), q), :] for start in (mine, mine + q, theirs, theirs + q)]


def first_back_call(idx, d_o, w_up, w1o, q, fe, bm):
    def load(r, k, wr, scr):
        pieces = [col_at(wr[0], (r * 2 + k) * fe, fe)] + list(wr[1:])
        return [list(zip(pieces, place_rows(r, q, scr[0])))]

    def step(arrive, tin, cr, tout, sr, scr):
        arrive(0)
        for j in range(2):
            y = mmt(tin[0][...], scr[0][2 * j * q:2 * (j + 1) * q, :])
            tout[2 * j][...] = y[:, :q]
            tout[2 * j + 1][...] = y[:, q:]

    flops = 2 * d_o.shape[0] * 4 * q * fe
    return tiled_call((load, step), idx, [(), ()], [d_o], [w_up] + list(w1o), [], [(q, f32)] * 4, [], [], [pltpu.VMEM((4 * q, fe), bf16)], bm, flops)


def back_call(idx, blocks, flat, w_up, w1n, w2n, q, fe, bm):
    dm = 4 * q

    def load(r, k, wr, scr):
        w1, w2 = scr
        first = [(p, w2.at[:, j * q:(j + 1) * q]) for j, p in enumerate(wr[4:])]
        pieces = [col_at(wr[0], ((1 - r) * 2 + k) * fe, fe)] + list(wr[1:4])
        return [first, list(zip(pieces, place_rows(r, q, w1)))]

    def step(arrive, tin, cr, tout, sr, scr):
        gu, gv, s_in = tin[:3]
        part = tin[3:]
        w1, w2 = scr
        dcn, outs = tout[0], tout[1:]
        arrive(0)
        for n0 in range(0, fe, CH_BACK):
            sl = slice(n0, n0 + CH_BACK)
            p = mmt(side(gu, gv), w2[sl, :]) * s_in[:, sl]
            dcn[:, sl] = p.astype(bf16)
            sr[0][:, sl] += jnp.sum(p, axis=0, keepdims=True)
        arrive(1)
        for j in range(2):
            y = mmt(dcn[...], w1[2 * j * q:2 * (j + 1) * q, :])
            outs[j][...] = part[2 * j][...] + y[:, :q]
            outs[2 + j][...] = part[2 * j + 1][...] + y[:, q:]

    flops = 2 * blocks[0][0].shape[0] * len(blocks) * dm * fe * 2
    return tiled_call((load, step), idx, blocks, flat, [w_up] + list(w1n) + list(w2n), [],
                      [(fe, bf16)] + [(q, f32)] * 2, [q, q], [(1, fe)], [pltpu.VMEM((dm, fe), bf16), pltpu.VMEM((fe, dm), bf16)], bm, flops)


def grad_call(idx, n, lhs, rhs, acc, out_dtype, halves):
    fe = rhs[0][0][0].shape[1]
    m = fe
    ng, nl, nblk = len(rhs), len(lhs[0]), len(lhs)
    ins, in_specs = [], []
    for parts in lhs:
        for p, b in parts:
            ins.append(p)
            if halves:
                in_specs.append(pl.BlockSpec((n, m // 2), functools.partial(lambda b, j, s: (b, s[0]), b), pipeline_mode=pl.Buffered(1)))
            else:
                in_specs.append(pl.BlockSpec((n, m), functools.partial(lambda b, j, s: (b, 0), b), pipeline_mode=pl.Buffered(1)))
    for parts in rhs:
        for p, b in parts:
            ins.append(p)
            in_specs.append(pl.BlockSpec((n, CH_GRAD), functools.partial(lambda b, j, s: (b, j), b)))
    used = [p for p in acc if p is not None]
    for p in used:
        ins.append(p)
        in_specs.append(pl.BlockSpec((m, CH_GRAD), lambda j, s: (0, j)))

    def kernel(idx_ref, *refs):
        refs = list(refs)
        lr = [refs.pop(0) for _ in range(nl * nblk)]
        rr = [[refs.pop(0) for _ in parts] for parts in rhs]
        ar = [None if p is None else refs.pop(0) for p in acc]
        outs, scr = refs[:ng], refs[ng]

        @pl.when(pl.program_id(0) == 0)
        def _():
            for b in range(nblk):
                for p in range(nl):
                    w = m // nl
                    scr[p * w:(p + 1) * w, b * n:(b + 1) * n] = lr[b * nl + p][...].T

        for g in range(ng):
            y = mm(scr[:, 0:len(rr[g]) * n], jnp.concatenate([v[...] for v in rr[g]], axis=0))
            if ar[g] is not None:
                y = y + ar[g][...]
            outs[g][...] = y.astype(out_dtype)

    return pl.pallas_call(
        kernel,
        out_shape=[jax.ShapeDtypeStruct((m, fe), out_dtype)] * ng,
        grid_spec=pltpu.PrefetchScalarGridSpec(
            num_scalar_prefetch=1, grid=(fe // CH_GRAD,), in_specs=in_specs,
            out_specs=[pl.BlockSpec((m, CH_GRAD), lambda j, s: (0, j))] * ng,
            scratch_shapes=[pltpu.VMEM((m, nblk * n), bf16)]),
        compiler_params=pltpu.CompilerParams(dimension_semantics=("arbitrary",), vmem_limit_bytes=VMEM_LIMIT),
        cost_estimate=pl.CostEstimate(flops=2 * n * m * fe * sum(len(p) for p in rhs), bytes_accessed=1 << 24, transcendentals=0),
    )(idx, *ins)


def final_grad_call(idx, n, lhs, rhs, acc, halves):
    fe = rhs[0][0][0].shape[1]
    nl, nblk, nt = len(lhs[0]), len(lhs), fe // CH_GRAD
    half = fe // 2

    def on(g, t):
        return jnp.clip(t - g * nt, 0, nt - 1)

    ins, in_specs = [], []
    for parts in lhs:
        for p, b in parts:
            ins.append(p)
            shape = (n, half) if halves else (n, fe)
            in_specs.append(pl.BlockSpec(shape, functools.partial(lambda b, t, s: (b, s[0] if halves else 0), b), pipeline_mode=pl.Buffered(1)))
    for g, parts in enumerate(rhs):
        for p, b in parts:
            ins.append(p)
            in_specs.append(pl.BlockSpec((n, CH_GRAD), functools.partial(lambda b, g, t, s: (b, on(g, t)), b, g)))
    for g, p in enumerate(acc):
        ins.append(p)
        in_specs.append(pl.BlockSpec((fe, CH_GRAD), functools.partial(lambda g, t, s: (0, on(g, t)), g)))
    if halves:
        outs = [jax.ShapeDtypeStruct((half, 4 * fe), bf16), jax.ShapeDtypeStruct((half, 2 * fe), bf16)]
        out_specs = [pl.BlockSpec((half, CH_GRAD), lambda t, s: (0, (jnp.where(t < nt, s[0], 1 - s[0]) * 2 + s[1]) * nt + t % nt)),
                     pl.BlockSpec((half, CH_GRAD), lambda t, s: (0, t))]
    else:
        outs = [jax.ShapeDtypeStruct((2 * fe, fe), bf16), jax.ShapeDtypeStruct((fe, fe), bf16)]
        out_specs = [pl.BlockSpec((fe, CH_GRAD), lambda t, s: (s[1], on(0, t))), pl.BlockSpec((fe, CH_GRAD), lambda t, s: (0, on(1, t)))]

    def kernel(idx_ref, *refs):
        refs = list(refs)
        lr = [refs.pop(0) for _ in range(nl * nblk)]
        rr = [[refs.pop(0) for _ in parts] for parts in rhs]
        ar = [refs.pop(0) for _ in acc]
        keep, send, scr = refs
        t = pl.program_id(0)

        @pl.when(t == 0)
        def _():
            for b in range(nblk):
                for p in range(nl):
                    w = fe // nl
                    scr[p * w:(p + 1) * w, b * n:(b + 1) * n] = lr[b * nl + p][...].T

        for g in range(2):
            @pl.when(t // nt == g)
            def _(g=g):
                y = mm(scr[...], jnp.concatenate([v[...] for v in rr[g]], axis=0)) + ar[g][...]
                if halves:
                    keep[...] = y[:half].astype(bf16)
                    send[...] = y[half:].astype(bf16)
                else:
                    (keep, send)[g][...] = y.astype(bf16)

    return pl.pallas_call(
        kernel,
        out_shape=outs,
        grid_spec=pltpu.PrefetchScalarGridSpec(
            num_scalar_prefetch=1, grid=(2 * nt,), in_specs=in_specs, out_specs=out_specs,
            scratch_shapes=[pltpu.VMEM((fe, nblk * n), bf16)]),
        compiler_params=pltpu.CompilerParams(dimension_semantics=("arbitrary",), vmem_limit_bytes=VMEM_LIMIT),
        cost_estimate=pl.CostEstimate(flops=4 * n * nblk * fe * fe, bytes_accessed=1 << 24, transcendentals=0),
    )(idx, *ins)


def solution(mesh):
    dep_size = mesh.shape["dep"]
    tok_spec = P(("part", "row", "col"), "dep")
    vec_dep = P("dep")
    part_dep = P(("part", "dep"))
    in_specs = (tok_spec, vec_dep, vec_dep, P(("dep", "row"), "col"), P("col"), P(("col", "row"), "dep"), vec_dep, tok_spec)
    out_specs = (tok_spec, tok_spec, P(("part", "dep", "row"), "col"), P(("part", "col")), P(("part", "col", "row"), "dep"), part_dep, part_dep, part_dep)

    def px(v):
        return lax.ppermute(v, "col", SWAP)

    def py(v):
        return lax.ppermute(v, "row", SWAP)

    def pd(v):
        return lax.ppermute(v, "dep", SWAP)

    def pyd(v):
        return lax.ppermute(v, ("row", "dep"), CROSS)

    def local_step(x_in, ln_scale, ln_shift, w_up, b_up, w_down, b_down, y_grad):
        r = lax.axis_index("row")
        k = lax.axis_index("dep")
        idx = jnp.stack([r, k]).astype(jnp.int32)
        n, dh_ = x_in.shape
        q = dh_ // 2
        fe = w_up.shape[1] // 4
        row_width = dh_ * dep_size

        def cols(rr, kk):
            return lax.dynamic_slice_in_dim(w_up, (rr * 2 + kk) * fe, fe, axis=1)

        def rows(kk):
            return lax.dynamic_slice_in_dim(w_down, kk * fe, fe, axis=0)

        def bias(rr):
            return lax.dynamic_slice_in_dim(b_up, (rr * 2 + k) * fe, fe, axis=0).astype(f32)

        gx = px(y_grad)
        own_o, own_n, snd_o, snd_n = cols(r, k), cols(1 - r, k), cols(r, 1 - k), cols(1 - r, 1 - k)
        w1o = (pd(snd_o), py(own_n), pyd(snd_n))
        w1n = (pd(snd_n), py(own_o), pyd(snd_o))
        rk, rk2 = rows(k), rows(1 - k)
        w2o = (pd(rk2),)
        own0, oth0 = py(rk[:, :q]), pyd(rk2[:, :q])
        own1, oth1 = py(rk[:, q:]), pyd(rk2[:, q:])
        w2n = (own0, own1, oth0, oth1)
        bo, bn = bias(r), bias(1 - r)

        x_float = x_in.astype(f32)
        row_stats = jnp.stack([jnp.sum(x_float, axis=1), jnp.sum(x_float * x_float, axis=1)], axis=1)
        row_stats = lax.psum(row_stats, "dep")
        mean_row = row_stats[:, 0:1] / row_width
        var_row = row_stats[:, 1:2] / row_width - mean_row * mean_row
        inv_std = lax.rsqrt(var_row + LN_EPS)
        x_hat = (x_float - mean_row) * inv_std
        a0 = (x_hat * ln_scale + ln_shift).astype(bf16)
        ax, ay = px(a0), py(a0)
        gy = py(y_grad)
        az, gz = px(ay), py(gx)

        def half(u):
            return (u, pd(u))

        A = [half(a0), half(ax), half(ay), half(az)]
        G = [half(y_grad), half(gx), half(gy), half(gz)]
        go, gn = (True, w1o, w2o, True), (False, w1n, w2n, True)

        def act(mode, blocks, slopes, groups, biases, sums):
            return act_call(mode, idx, blocks, slopes, groups, w_up, w_down, biases, 256, sums)

        def grad(*args):
            return grad_call(idx, n, *args)

        def whole(pair):
            return [(pair[0], 0), (pair[1], 0)]

        A0, A1, A2, A3 = [whole(p) for p in A]

        h_o, d_o, sum_o = act("cd", [A[0] + G[0], A[1] + G[1]], [], [go], [bo], True)
        h_n, s_n = act("c", [A[0], A[1]], [], [gn], [bn], False)
        two_o, two_g = [(d_o, 0), (d_o, 1)], [[(G[0][p], 0), (G[1][p], 0)] for p in range(2)]
        dw2 = grad([[(h_o, 0)], [(h_o, 1)]], two_g, [None, None], f32, False)
        dw1o, = grad([A0, A1], [two_o], [None], f32, True)
        gn_s = (False, w1n, w2n, False)
        hy, syo, syn = act("c", [A[2]], [], [go, gn_s], [bo, bn], False)
        hz, szo, szn = act("c", [A[3]], [], [go, gn_s], [bo, bn], False)

        def reduce_out(own, oth):
            oth_a, oth_x = oth
            send = own[n:] + pd(oth_x)
            return own[:n] + pd(oth_a) + px(send)

        def local_copies(j, kk, down, dep, buf):
            return [(down.at[pl.ds(pl.multiple_of(kk * fe, 8), fe), j * q:(j + 1) * q], buf.at[0:fe, 0:q]), (dep.at[:, j * q:(j + 1) * q], buf.at[0:fe, q:2 * q])]

        def far_copies(start, a, b, buf):
            return [(a, buf.at[start:start + fe, 0:q]), (b, buf.at[start:start + fe, q:2 * q])]

        def y_first(rr, kk, wr, buf):
            return local_copies(0, kk, wr[0], wr[1], buf) + far_copies(fe, wr[2], wr[3], buf)

        def out(*args):
            return out_call(idx, *args, 256)

        def y_finish(j, val):
            cs = slice(j * q, (j + 1) * q)
            return (x_in[:, cs].astype(f32) + val + b_down[cs].astype(f32)).astype(bf16)

        res = out([h_o, h_n], [], [w_down, w2o[0], own0, oth0], y_first, q, True)
        y0 = y_finish(0, reduce_out(res[0], res[1:]))
        y1o = out([h_o], [], [w_down, w2o[0]], lambda rr, kk, wr, buf: local_copies(1, kk, wr[0], wr[1], buf), q, False)
        res = out([h_n], y1o, [own1, oth1], lambda rr, kk, wr, buf: far_copies(0, wr[0], wr[1], buf), q, True)
        y1 = y_finish(1, reduce_out(res[0], res[1:]))
        y_out = jnp.concatenate([y0, y1], axis=1)

        da_o = first_back_call(idx, d_o, w_up, w1o, q, fe, 256)
        d_n, own_a, own_b, *oth, sum_n = back_call(idx, [G[0], G[1]], [s_n] + list(da_o), w_up, w1n, w2n, q, fe, 256)
        na = reduce_out(own_a, oth[:2])
        nb = reduce_out(own_b, oth[2:])
        norm_grad = jnp.concatenate([na, nb], axis=1)
        value = norm_grad * ln_scale
        grad_stats = jnp.stack([jnp.sum(value, axis=1), jnp.sum(value * x_hat, axis=1)], axis=1)
        grad_stats = lax.psum(grad_stats, "dep")
        dx = inv_std * (value - grad_stats[:, 0:1] / row_width - x_hat * (grad_stats[:, 1:2] / row_width))
        x_grad = (y_grad.astype(f32) + dx).astype(bf16)
        gains = jnp.stack([jnp.sum(norm_grad * x_hat, axis=0), jnp.sum(norm_grad, axis=0)])

        dw1n, = grad([A0, A1], [[(d_n, 0), (d_n, 1)]], [None], f32, True)
        fy = act("d", [G[2]], [syo, syn], [go, gn], [], False)
        fz = act("d", [G[3]], [szo, szn], [go, gn], [], False)
        far_g = [[(G[2][p], 0), (G[3][p], 0)] for p in range(2)]
        w_up_grad, send1 = final_grad_call(idx, n, [A2, A3], [[(fy[g], 0), (fz[g], 0)] for g in range(2)], [dw1o, dw1n], True)
        w_down_grad, send2 = final_grad_call(idx, n, [[(hy, 0)], [(hz, 0)]], far_g, dw2, False)
        got1, got2 = pd(send1), pd(send2)
        for g, rr in enumerate((r, 1 - r)):
            w_up_grad = lax.dynamic_update_slice_in_dim(w_up_grad, got1[:, g * fe:(g + 1) * fe], (rr * 2 + 1 - k) * fe, axis=1)
        w_down_grad = lax.dynamic_update_slice_in_dim(w_down_grad, got2, (1 - k) * fe, axis=0)

        def both(v):
            v = v + px(v)
            return v + py(v)

        b_down_grad = both(jnp.sum(y_grad.astype(f32), axis=0))
        gain_sums = both(gains)
        full = jnp.concatenate([sum_o, sum_n]) + py(jnp.concatenate([sum_n, sum_o]))
        oth = pd(full)
        b_up_grad = jnp.zeros(b_up.shape, f32)
        for v, rr, kk in ((full[0], r, k), (full[1], 1 - r, k), (oth[0], r, 1 - k), (oth[1], 1 - r, 1 - k)):
            b_up_grad = lax.dynamic_update_slice_in_dim(b_up_grad, v, (rr * 2 + kk) * fe, axis=0)
        return (y_out, x_grad, w_up_grad, b_up_grad, w_down_grad, b_down_grad, gain_sums[0], gain_sums[1])

    return jax.shard_map(local_step, mesh=mesh, in_specs=in_specs, out_specs=out_specs, check_vma=False)
```

```python
import functools
import jax
import jax.numpy as jnp
from jax import lax
from jax.experimental import pallas as pl
from jax.experimental.pallas import tpu as pltpu
from jax.sharding import PartitionSpec as P

LN_EPS = 1e-5
GELU_K = 0.7978845608028654
GELU_C = 0.044715
SWAP = [(0, 1), (1, 0)]
CROSS = [(0, 3), (1, 2), (2, 1), (3, 0)]
f32 = jnp.float32
bf16 = jnp.bfloat16
VMEM_LIMIT = 60 * 1024 * 1024
CH_ACT = 256
CH_BACK = 640
CH_GRAD = 256


def gelu_both(c):
    sq = c * c
    t = jnp.tanh(c * (GELU_K + (GELU_K * GELU_C) * sq))
    half = 0.5 * c
    h = half + half * t
    s = (0.5 + 0.5 * t) + half * (1.0 - t * t) * (GELU_K + (3.0 * GELU_K * GELU_C) * sq)
    return h, s


def mm(a, b):
    return lax.dot_general(a, b, (((1,), (0,)), ((), ())), preferred_element_type=f32)


def mmt(a, b):
    return lax.dot_general(a, b, (((1,), (1,)), ((), ())), preferred_element_type=f32)


def side(u, v):
    return jnp.concatenate([u[...], v[...]], axis=1)


def copies_of(stages, sems):
    at, out = 0, []
    for stage in stages:
        out.append([pltpu.make_async_copy(s, d, sems.at[at + i]) for i, (s, d) in enumerate(stage)])
        at += len(stage)
    return out


def tile_map(b, nb, i, *_):
    return (jnp.clip(i - b * nb, 0, nb - 1), 0)


HBM = pl.BlockSpec(memory_space=pl.ANY)


def tiled_call(body, idx, pieces, flat, weights, consts, flat_out, part_out, sums_out, scratch, bm, flops):
    nblk = len(pieces)
    n = (flat[0] if flat else pieces[0][0]).shape[0] // (nblk if flat else 1)
    nb = n // bm
    ins, in_specs, outs, out_specs = [], [], [], []
    for b, arrs in enumerate(pieces):
        for a in arrs:
            ins.append(a)
            in_specs.append(pl.BlockSpec((bm, a.shape[1]), functools.partial(tile_map, b, nb)))
    for a in flat:
        ins.append(a)
        in_specs.append(pl.BlockSpec((bm, a.shape[1]), lambda i, *_: (i, 0)))
    for w in weights:
        ins.append(w)
        in_specs.append(HBM)
    for c in consts:
        ins.append(c)
        in_specs.append(pl.BlockSpec(c.shape, lambda i, *_: (0, 0)))
    for shp in flat_out:
        outs.append(jax.ShapeDtypeStruct((n * nblk, shp[0]), shp[1]))
        out_specs.append(pl.BlockSpec((bm, shp[0]), lambda i, *_: (i, 0)))
    for width in part_out:
        for b in range(nblk):
            outs.append(jax.ShapeDtypeStruct((n, width), f32))
            out_specs.append(pl.BlockSpec((bm, width), functools.partial(tile_map, b, nb)))
    for shp in sums_out:
        outs.append(jax.ShapeDtypeStruct(shp, f32))
        out_specs.append(pl.BlockSpec(shp, lambda i, *_: (0, 0)))
    na = len(pieces[0])

    def kernel(idx_ref, *refs):
        i = pl.program_id(0)
        at = na * nblk
        fl = refs[at:at + len(flat)]
        tin = [refs[b * na:(b + 1) * na] + fl for b in range(nblk)]
        at += len(flat)
        wr = refs[at:at + len(weights)]
        at += len(weights)
        cr = refs[at:at + len(consts)]
        at += len(consts)
        tout = refs[at:at + len(flat_out)]
        at += len(flat_out)
        pout = refs[at:at + len(part_out) * nblk]
        at += len(part_out) * nblk
        sr = refs[at:at + len(sums_out)]
        at += len(sums_out)
        scr, sems = refs[at:-1], refs[-1]
        load, step = body

        @pl.when(i == 0)
        def _():
            for stage in copies_of(load(idx_ref[0], idx_ref[1], wr, scr), sems):
                for c in stage:
                    c.start()
            for s in sr:
                s[...] = jnp.zeros_like(s)

        def arrive(j):
            @pl.when(i == 0)
            def _():
                for c in copies_of(load(idx_ref[0], idx_ref[1], wr, scr), sems)[j]:
                    c.wait()

        for b in range(nblk):
            @pl.when(i // nb == b)
            def _(b=b):
                step(arrive if b == 0 else lambda j: None, tin[b], cr, tout + pout[b::nblk], sr, scr)

    call = pl.pallas_call(
        kernel,
        out_shape=outs,
        grid_spec=pltpu.PrefetchScalarGridSpec(
            num_scalar_prefetch=1, grid=(nblk * nb,), in_specs=in_specs, out_specs=out_specs,
            scratch_shapes=list(scratch) + [pltpu.SemaphoreType.DMA((32,))]),
        compiler_params=pltpu.CompilerParams(dimension_semantics=("arbitrary",), vmem_limit_bytes=VMEM_LIMIT),
        cost_estimate=pl.CostEstimate(flops=flops, bytes_accessed=1 << 24, transcendentals=0),
    )
    return call(idx, *ins)


def col_at(ref, start, size):
    return ref.at[:, pl.ds(pl.multiple_of(start, 128), size)]


def row_at(ref, start, size):
    return ref.at[pl.ds(pl.multiple_of(start, 8), size), :]


def act_call(mode, idx, blocks, slopes, groups, w_up, w_down, biases, bm, with_sums):
    fe = w_up.shape[1] // 4
    q = w_up.shape[0]
    dm = 4 * q
    ng = len(groups)
    has_c, has_d = "c" in mode, mode in ("d", "r")
    weights = [w_up, w_down]
    for _, p1, p2, _ in groups:
        weights += (list(p1) if has_c else []) + (list(p2) if has_d else [])

    def load(r, k, wr, scr):
        up, down = wr[0], wr[1]
        rest = list(wr[2:])
        bufs = list(scr)
        stages = []
        for own, p1, p2, _ in groups:
            copies = []
            if has_c:
                buf = bufs.pop(0)
                rr = r if own else 1 - r
                dep, row, cross = rest.pop(0), rest.pop(0), rest.pop(0)
                copies += [(col_at(up, (rr * 2 + k) * fe, fe), row_at(buf, r * q, q)),
                           (row, row_at(buf, (1 - r) * q, q)),
                           (dep, row_at(buf, 2 * q + r * q, q)),
                           (cross, row_at(buf, 2 * q + (1 - r) * q, q))]
            if has_d:
                buf = bufs.pop(0)
                if own:
                    dep = rest.pop(0)
                    copies += [(row_at(down, k * fe, fe), buf.at[:, 0:2 * q]), (dep, buf.at[:, 2 * q:4 * q])]
                else:
                    for j in range(4):
                        copies.append((rest.pop(0), buf.at[:, j * q:(j + 1) * q]))
            stages.append(copies)
        return stages

    def step(arrive, tin, cr, tout, sr, scr):
        tin, bufs = list(tin), list(scr)
        u, v = (tin.pop(0), tin.pop(0)) if has_c else (None, None)
        gu, gv = (tin.pop(0), tin.pop(0)) if has_d else (None, None)
        tout = list(tout)
        for g in range(ng):
            arrive(g)
            w1 = bufs.pop(0) if has_c else None
            w2 = bufs.pop(0) if has_d else None
            extra = tin.pop(0) if mode in ("d", "ce") else None
            h_out = tout.pop(0) if has_c and groups[g][3] else None
            x_out = tout.pop(0)
            for n0 in range(0, fe, CH_ACT):
                sl = slice(n0, n0 + CH_ACT)
                if has_c:
                    c = mm(side(u, v), w1[:, sl]) + cr[g][:, sl]
                    h, p = gelu_both(c)
                    if h_out is not None:
                        h_out[:, sl] = h.astype(bf16)
                else:
                    p = mmt(side(gu, gv), w2[sl, :])
                if extra is not None:
                    p = p * extra[:, sl]
                x_out[:, sl] = p.astype(x_out.dtype)
                if with_sums:
                    sr[g][:, sl] += jnp.sum(p, axis=0, keepdims=True)

    scratch = []
    for _ in range(ng):
        scratch += [pltpu.VMEM((dm, fe), bf16)] if has_c else []
        scratch += [pltpu.VMEM((fe, dm), bf16)] if has_d else []
    outs = []
    for g in range(ng):
        outs += [(fe, bf16)] if has_c and groups[g][3] else []
        outs += [(fe, bf16)] if mode in ("d", "ce") else [(fe, f32)]
    n = blocks[0][0].shape[0]
    flops = 2 * n * len(blocks) * dm * fe * ng * (int(has_c) + int(has_d))
    res = tiled_call((load, step), idx, blocks, slopes, weights, [b.reshape(1, fe) for b in biases] if has_c else [],
                     outs, [], [(1, fe)] * ng if with_sums else [], scratch, bm, flops)
    return res


def out_call(idx, lhs, acc, weights, load_fn, q, last, bm):
    depth = sum(a.shape[1] for a in lhs)

    def load(r, k, wr, scr):
        return [load_fn(r, k, wr, scr[0])]

    def step(arrive, tin, cr, tout, sr, scr):
        arrive(0)
        y = mm(jnp.concatenate([a[...] for a in tin[:len(lhs)]], axis=1), scr[0][...])
        for p in range(2):
            v = y[:, p * q:(p + 1) * q]
            tout[p][...] = v + tin[len(lhs) + p][...] if acc else v

    flops = 2 * lhs[0].shape[0] * 2 * q * depth
    return tiled_call((load, step), idx, [(), ()], list(lhs) + list(acc), weights, [], [(q, f32)] * (1 if last else 2), [q] if last else [], [],
                      [pltpu.VMEM((depth, 2 * q), bf16)], bm, flops)


def place_rows(r, q, buf):
    mine, theirs = r * 2 * q, (1 - r) * 2 * q
    return [buf.at[pl.ds(pl.multiple_of(start, 8), q), :] for start in (mine, mine + q, theirs, theirs + q)]


def first_back_call(idx, d_o, w_up, w1o, q, fe, bm):
    def load(r, k, wr, scr):
        pieces = [col_at(wr[0], (r * 2 + k) * fe, fe)] + list(wr[1:])
        return [list(zip(pieces, place_rows(r, q, scr[0])))]

    def step(arrive, tin, cr, tout, sr, scr):
        arrive(0)
        for j in range(2):
            y = mmt(tin[0][...], scr[0][2 * j * q:2 * (j + 1) * q, :])
            tout[2 * j][...] = y[:, :q]
            tout[2 * j + 1][...] = y[:, q:]

    flops = 2 * d_o.shape[0] * 4 * q * fe
    return tiled_call((load, step), idx, [(), ()], [d_o], [w_up] + list(w1o), [], [(q, f32)] * 4, [], [], [pltpu.VMEM((4 * q, fe), bf16)], bm, flops)


def back_call(idx, blocks, flat, w_up, w1n, w2n, q, fe, bm):
    dm = 4 * q

    def load(r, k, wr, scr):
        w1, w2 = scr
        first = [(p, w2.at[:, j * q:(j + 1) * q]) for j, p in enumerate(wr[4:])]
        pieces = [col_at(wr[0], ((1 - r) * 2 + k) * fe, fe)] + list(wr[1:4])
        return [first, list(zip(pieces, place_rows(r, q, w1)))]

    def step(arrive, tin, cr, tout, sr, scr):
        gu, gv, s_in = tin[:3]
        part = tin[3:]
        w1, w2 = scr
        dcn, outs = tout[0], tout[1:]
        arrive(0)
        for n0 in range(0, fe, CH_BACK):
            sl = slice(n0, n0 + CH_BACK)
            p = mmt(side(gu, gv), w2[sl, :]) * s_in[:, sl]
            dcn[:, sl] = p.astype(bf16)
            sr[0][:, sl] += jnp.sum(p, axis=0, keepdims=True)
        arrive(1)
        for j in range(2):
            y = mmt(dcn[...], w1[2 * j * q:2 * (j + 1) * q, :])
            outs[j][...] = part[2 * j][...] + y[:, :q]
            outs[2 + j][...] = part[2 * j + 1][...] + y[:, q:]

    flops = 2 * blocks[0][0].shape[0] * len(blocks) * dm * fe * 2
    return tiled_call((load, step), idx, blocks, flat, [w_up] + list(w1n) + list(w2n), [],
                      [(fe, bf16)] + [(q, f32)] * 2, [q, q], [(1, fe)], [pltpu.VMEM((dm, fe), bf16), pltpu.VMEM((fe, dm), bf16)], bm, flops)


def grad_call(idx, n, lhs, rhs, acc, out_dtype, halves):
    fe = rhs[0][0][0].shape[1]
    m = fe
    ng, nl, nblk = len(rhs), len(lhs[0]), len(lhs)
    ins, in_specs = [], []
    for parts in lhs:
        for p, b in parts:
            ins.append(p)
            if halves:
                in_specs.append(pl.BlockSpec((n, m // 2), functools.partial(lambda b, j, s: (b, s[0]), b), pipeline_mode=pl.Buffered(1)))
            else:
                in_specs.append(pl.BlockSpec((n, m), functools.partial(lambda b, j, s: (b, 0), b), pipeline_mode=pl.Buffered(1)))
    for parts in rhs:
        for p, b in parts:
            ins.append(p)
            in_specs.append(pl.BlockSpec((n, CH_GRAD), functools.partial(lambda b, j, s: (b, j), b)))
    used = [p for p in acc if p is not None]
    for p in used:
        ins.append(p)
        in_specs.append(pl.BlockSpec((m, CH_GRAD), lambda j, s: (0, j)))

    def kernel(idx_ref, *refs):
        refs = list(refs)
        lr = [refs.pop(0) for _ in range(nl * nblk)]
        rr = [[refs.pop(0) for _ in parts] for parts in rhs]
        ar = [None if p is None else refs.pop(0) for p in acc]
        outs, scr = refs[:ng], refs[ng]

        @pl.when(pl.program_id(0) == 0)
        def _():
            for b in range(nblk):
                for p in range(nl):
                    w = m // nl
                    scr[p * w:(p + 1) * w, b * n:(b + 1) * n] = lr[b * nl + p][...].T

        for g in range(ng):
            y = mm(scr[:, 0:len(rr[g]) * n], jnp.concatenate([v[...] for v in rr[g]], axis=0))
            if ar[g] is not None:
                y = y + ar[g][...]
            outs[g][...] = y.astype(out_dtype)

    return pl.pallas_call(
        kernel,
        out_shape=[jax.ShapeDtypeStruct((m, fe), out_dtype)] * ng,
        grid_spec=pltpu.PrefetchScalarGridSpec(
            num_scalar_prefetch=1, grid=(fe // CH_GRAD,), in_specs=in_specs,
            out_specs=[pl.BlockSpec((m, CH_GRAD), lambda j, s: (0, j))] * ng,
            scratch_shapes=[pltpu.VMEM((m, nblk * n), bf16)]),
        compiler_params=pltpu.CompilerParams(dimension_semantics=("arbitrary",), vmem_limit_bytes=VMEM_LIMIT),
        cost_estimate=pl.CostEstimate(flops=2 * n * m * fe * sum(len(p) for p in rhs), bytes_accessed=1 << 24, transcendentals=0),
    )(idx, *ins)


def final_grad_call(idx, n, lhs, rhs, acc, halves):
    fe = rhs[0][0][0].shape[1]
    nl, nblk, nt = len(lhs[0]), len(lhs), fe // CH_GRAD
    half = fe // 2

    def on(g, t):
        return jnp.clip(t - g * nt, 0, nt - 1)

    ins, in_specs = [], []
    for parts in lhs:
        for p, b in parts:
            ins.append(p)
            shape = (n, half) if halves else (n, fe)
            in_specs.append(pl.BlockSpec(shape, functools.partial(lambda b, t, s: (b, s[0] if halves else 0), b), pipeline_mode=pl.Buffered(1)))
    for g, parts in enumerate(rhs):
        for p, b in parts:
            ins.append(p)
            in_specs.append(pl.BlockSpec((n, CH_GRAD), functools.partial(lambda b, g, t, s: (b, on(g, t)), b, g)))
    for g, p in enumerate(acc):
        ins.append(p)
        in_specs.append(pl.BlockSpec((fe, CH_GRAD), functools.partial(lambda g, t, s: (0, on(g, t)), g)))
    if halves:
        outs = [jax.ShapeDtypeStruct((half, 4 * fe), bf16), jax.ShapeDtypeStruct((half, 2 * fe), bf16)]
        out_specs = [pl.BlockSpec((half, CH_GRAD), lambda t, s: (0, (jnp.where(t < nt, s[0], 1 - s[0]) * 2 + s[1]) * nt + t % nt)),
                     pl.BlockSpec((half, CH_GRAD), lambda t, s: (0, t))]
    else:
        outs = [jax.ShapeDtypeStruct((2 * fe, fe), bf16), jax.ShapeDtypeStruct((fe, fe), bf16)]
        out_specs = [pl.BlockSpec((fe, CH_GRAD), lambda t, s: (s[1], on(0, t))), pl.BlockSpec((fe, CH_GRAD), lambda t, s: (0, on(1, t)))]

    def kernel(idx_ref, *refs):
        refs = list(refs)
        lr = [refs.pop(0) for _ in range(nl * nblk)]
        rr = [[refs.pop(0) for _ in parts] for parts in rhs]
        ar = [refs.pop(0) for _ in acc]
        keep, send, scr = refs
        t = pl.program_id(0)

        @pl.when(t == 0)
        def _():
            for b in range(nblk):
                for p in range(nl):
                    w = fe // nl
                    scr[p * w:(p + 1) * w, b * n:(b + 1) * n] = lr[b * nl + p][...].T

        for g in range(2):
            @pl.when(t // nt == g)
            def _(g=g):
                y = mm(scr[...], jnp.concatenate([v[...] for v in rr[g]], axis=0)) + ar[g][...]
                if halves:
                    keep[...] = y[:half].astype(bf16)
                    send[...] = y[half:].astype(bf16)
                else:
                    (keep, send)[g][...] = y.astype(bf16)

    return pl.pallas_call(
        kernel,
        out_shape=outs,
        grid_spec=pltpu.PrefetchScalarGridSpec(
            num_scalar_prefetch=1, grid=(2 * nt,), in_specs=in_specs, out_specs=out_specs,
            scratch_shapes=[pltpu.VMEM((fe, nblk * n), bf16)]),
        compiler_params=pltpu.CompilerParams(dimension_semantics=("arbitrary",), vmem_limit_bytes=VMEM_LIMIT),
        cost_estimate=pl.CostEstimate(flops=4 * n * nblk * fe * fe, bytes_accessed=1 << 24, transcendentals=0),
    )(idx, *ins)


def solution(mesh):
    dep_size = mesh.shape["dep"]
    tok_spec = P(("part", "row", "col"), "dep")
    vec_dep = P("dep")
    part_dep = P(("part", "dep"))
    in_specs = (tok_spec, vec_dep, vec_dep, P(("dep", "row"), "col"), P("col"), P(("col", "row"), "dep"), vec_dep, tok_spec)
    out_specs = (tok_spec, tok_spec, P(("part", "dep", "row"), "col"), P(("part", "col")), P(("part", "col", "row"), "dep"), part_dep, part_dep, part_dep)

    def px(v):
        return lax.ppermute(v, "col", SWAP)

    def py(v):
        return lax.ppermute(v, "row", SWAP)

    def pd(v):
        return lax.ppermute(v, "dep", SWAP)

    def pyd(v):
        return lax.ppermute(v, ("row", "dep"), CROSS)

    def local_step(x_in, ln_scale, ln_shift, w_up, b_up, w_down, b_down, y_grad):
        r = lax.axis_index("row")
        k = lax.axis_index("dep")
        idx = jnp.stack([r, k]).astype(jnp.int32)
        n, dh_ = x_in.shape
        q = dh_ // 2
        fe = w_up.shape[1] // 4
        row_width = dh_ * dep_size

        def cols(w, rr, kk):
            return lax.dynamic_slice_in_dim(w, (rr * 2 + kk) * fe, fe, axis=1)

        def rows(kk):
            return lax.dynamic_slice_in_dim(w_down, kk * fe, fe, axis=0)

        def bias(rr):
            return lax.dynamic_slice_in_dim(b_up, (rr * 2 + k) * fe, fe, axis=0).astype(f32)

        gx = px(y_grad)
        own_n = cols(w_up, 1 - r, k)
        w_rest, own_n = lax.optimization_barrier((w_up, own_n))
        own_o, snd_o, snd_n = cols(w_rest, r, k), cols(w_rest, r, 1 - k), cols(w_rest, 1 - r, 1 - k)
        w1o = (pd(snd_o), py(own_n), pyd(snd_n))
        w1n = (pd(snd_n), py(own_o), pyd(snd_o))
        rk, rk2 = rows(k), rows(1 - k)
        w2o = (pd(rk2),)
        own0, oth0 = py(rk[:, :q]), pyd(rk2[:, :q])
        own1, oth1 = py(rk[:, q:]), pyd(rk2[:, q:])
        w2n = (own0, own1, oth0, oth1)
        bo, bn = bias(r), bias(1 - r)

        x_float = x_in.astype(f32)
        row_stats = jnp.stack([jnp.sum(x_float, axis=1), jnp.sum(x_float * x_float, axis=1)], axis=1)
        row_stats = lax.psum(row_stats, "dep")
        mean_row = row_stats[:, 0:1] / row_width
        var_row = row_stats[:, 1:2] / row_width - mean_row * mean_row
        inv_std = lax.rsqrt(var_row + LN_EPS)
        x_hat = (x_float - mean_row) * inv_std
        a0 = (x_hat * ln_scale + ln_shift).astype(bf16)
        ax, ay = px(a0), py(a0)
        gy = py(y_grad)
        az, gz = px(ay), py(gx)

        def half(u):
            return (u, pd(u))

        A = [half(a0), half(ax), half(ay), half(az)]
        G = [half(y_grad), half(gx), half(gy), half(gz)]
        go, gn = (True, w1o, w2o, True), (False, w1n, w2n, True)

        def act(mode, blocks, slopes, groups, biases, sums):
            return act_call(mode, idx, blocks, slopes, groups, w_up, w_down, biases, 256, sums)

        def grad(*args):
            return grad_call(idx, n, *args)

        def whole(pair):
            return [(pair[0], 0), (pair[1], 0)]

        A0, A1, A2, A3 = [whole(p) for p in A]

        dh_o, = act("r", [G[0], G[1]], [], [go], [], False)
        h_o, d_o, sum_o = act("ce", [A[0], A[1]], [dh_o], [go], [bo], True)
        h_n, s_n = act("c", [A[0], A[1]], [], [gn], [bn], False)
        two_o, two_g = [(d_o, 0), (d_o, 1)], [[(G[0][p], 0), (G[1][p], 0)] for p in range(2)]
        dw2 = grad([[(h_o, 0)], [(h_o, 1)]], two_g, [None, None], f32, False)
        dw1o, = grad([A0, A1], [two_o], [None], f32, True)
        gn_s = (False, w1n, w2n, False)
        hy, syo, syn = act("c", [A[2]], [], [go, gn_s], [bo, bn], False)
        hz, szo, szn = act("c", [A[3]], [], [go, gn_s], [bo, bn], False)

        def reduce_out(own, oth):
            oth_a, oth_x = oth
            send = own[n:] + pd(oth_x)
            return own[:n] + pd(oth_a) + px(send)

        def local_copies(j, kk, down, dep, buf):
            return [(down.at[pl.ds(pl.multiple_of(kk * fe, 8), fe), j * q:(j + 1) * q], buf.at[0:fe, 0:q]), (dep.at[:, j * q:(j + 1) * q], buf.at[0:fe, q:2 * q])]

        def far_copies(start, a, b, buf):
            return [(a, buf.at[start:start + fe, 0:q]), (b, buf.at[start:start + fe, q:2 * q])]

        def y_first(rr, kk, wr, buf):
            return local_copies(0, kk, wr[0], wr[1], buf) + far_copies(fe, wr[2], wr[3], buf)

        def out(*args):
            return out_call(idx, *args, 256)

        def y_finish(j, val):
            cs = slice(j * q, (j + 1) * q)
            return (x_in[:, cs].astype(f32) + val + b_down[cs].astype(f32)).astype(bf16)

        res = out([h_o, h_n], [], [w_down, w2o[0], own0, oth0], y_first, q, True)
        y0 = y_finish(0, reduce_out(res[0], res[1:]))
        y1o = out([h_o], [], [w_down, w2o[0]], lambda rr, kk, wr, buf: local_copies(1, kk, wr[0], wr[1], buf), q, False)
        res = out([h_n], y1o, [own1, oth1], lambda rr, kk, wr, buf: far_copies(0, wr[0], wr[1], buf), q, True)
        y1 = y_finish(1, reduce_out(res[0], res[1:]))
        y_out = jnp.concatenate([y0, y1], axis=1)

        da_o = first_back_call(idx, d_o, w_up, w1o, q, fe, 256)
        d_n, own_a, own_b, *oth, sum_n = back_call(idx, [G[0], G[1]], [s_n] + list(da_o), w_up, w1n, w2n, q, fe, 256)
        na = reduce_out(own_a, oth[:2])
        nb = reduce_out(own_b, oth[2:])
        norm_grad = jnp.concatenate([na, nb], axis=1)
        value = norm_grad * ln_scale
        grad_stats = jnp.stack([jnp.sum(value, axis=1), jnp.sum(value * x_hat, axis=1)], axis=1)
        grad_stats = lax.psum(grad_stats, "dep")
        dx = inv_std * (value - grad_stats[:, 0:1] / row_width - x_hat * (grad_stats[:, 1:2] / row_width))
        x_grad = (y_grad.astype(f32) + dx).astype(bf16)
        gains = jnp.stack([jnp.sum(norm_grad * x_hat, axis=0), jnp.sum(norm_grad, axis=0)])

        dw1n, = grad([A0, A1], [[(d_n, 0), (d_n, 1)]], [None], f32, True)
        far = act("d", [G[2] + (syo, syn), G[3] + (szo, szn)], [], [go, gn], [], False)
        far_g = [[(G[2][p], 0), (G[3][p], 0)] for p in range(2)]
        w_up_grad, send1 = final_grad_call(idx, n, [A2, A3], [[(far[g], 0), (far[g], 1)] for g in range(2)], [dw1o, dw1n], True)
        w_down_grad, send2 = final_grad_call(idx, n, [[(hy, 0)], [(hz, 0)]], far_g, dw2, False)
        got1, got2 = pd(send1), pd(send2)
        for g, rr in enumerate((r, 1 - r)):
            w_up_grad = lax.dynamic_update_slice_in_dim(w_up_grad, got1[:, g * fe:(g + 1) * fe], (rr * 2 + 1 - k) * fe, axis=1)
        w_down_grad = lax.dynamic_update_slice_in_dim(w_down_grad, got2, (1 - k) * fe, axis=0)

        def both(v):
            near, far = px(v), py(v)
            cross = lax.ppermute(v, ("row", "col"), CROSS)
            return (v + near) + (far + cross)

        b_down_grad = both(jnp.sum(y_grad.astype(f32), axis=0))
        gain_sums = both(gains)
        full = jnp.concatenate([sum_o, sum_n]) + py(jnp.concatenate([sum_n, sum_o]))
        oth = pd(full)
        b_up_grad = jnp.zeros(b_up.shape, f32)
        for v, rr, kk in ((full[0], r, k), (full[1], 1 - r, k), (oth[0], r, 1 - k), (oth[1], 1 - r, 1 - k)):
            b_up_grad = lax.dynamic_update_slice_in_dim(b_up_grad, v, (rr * 2 + kk) * fe, axis=0)
        return (y_out, x_grad, w_up_grad, b_up_grad, w_down_grad, b_down_grad, gain_sums[0], gain_sums[1])

    return jax.shard_map(local_step, mesh=mesh, in_specs=in_specs, out_specs=out_specs, check_vma=False)
```
